32 devices in a mesh: dp: 4 (over x, core), section: 2 (over y), tensor: 4 (over z).
Axes of the slice: x: 2, y: 2, z: 4, core: 2. Of those that a mesh axis runs over, the one named last changes fastest.
Arguments:
- observed: float32 [4, 2, 4, 2646], P('dp', 'section', 'tensor'), may hold values from 0.25 to 8
- section_of: int32 [126], replicated, may hold values from 0 to 1, as said below
- hist_len: int32 [21], replicated, may hold values from 1 to 127
- roll_index: int32 [], replicated, may hold values from 0 to 127
- history: float32 [128, 2646], replicated, may hold values from 0.02 to 64
- acts: bfloat16 [2, 1536, 16384], P('section', 'dp', 'tensor'), may hold values from -6 to 6
- grads: bfloat16 [2, 1536, 1024], P('section', 'dp', 'tensor'), may hold values from -6 to 6
Outputs:
- new_history: float32 [128, 2646], replicated
- new_scale: float32 [2646], replicated
- wgrad: bfloat16 [2, 16384, 1024], P('section', ('tensor', 'dp'))
The draws below stay inside these ranges and needn't reach their ends.
Inputs may be any that keep to these rules, and one draw needn't show every extreme that they name: `section_of`: layers are assigned to sections in contiguous ascending groups, and every section holds at least one layer.
All inputs are finite; a program needn't handle non-finite values.
Results may differ from the reference program's by a relative error of at most 0.017.
Values may be sent and summed in bfloat16 or wider, within the bound.
A program may use at most 64 MiB of HBM per device.

```python
import math
import jax
import jax.numpy as jnp
from jax import lax

D = 16384
KV = 1024
LAYERS = 126
NT = 21
HIST = 128
TOK_DEV = 384
TOKENS = 1536
LT = 2646
N_DP = 4
N_SECTION = 2
N_TENSOR = 4


def draw_section_of(key, part):
    cuts = jax.random.permutation(key, LAYERS - 1)[:N_SECTION - 1] + 1
    layer_ids = jnp.arange(LAYERS, dtype=jnp.int32)
    return jnp.sum((layer_ids[:, None] >= cuts[None, :]).astype(jnp.int32), axis=1).astype(jnp.int32)


def with_ends(values, key, low, high):
    longest = values.shape.index(max(values.shape))
    spots = []
    for shift in (0, 1):
        where = [jax.random.randint(jax.random.fold_in(key, axis), (), 0, length) for axis, length in enumerate(values.shape)]
        where[longest] = (where[longest] + shift) % values.shape[longest]
        spots.append(tuple(where))
    return values.at[spots[0]].set(low).at[spots[1]].set(high)


def block_levels(stream_key, dims, split, low, high):
    gain = 1.0
    for dim, parts in split:
        steps = jax.random.uniform(jax.random.fold_in(jax.random.fold_in(stream_key, 6), dim), (parts,), jnp.float32, low / len(split), high / len(split))
        gain = gain * jnp.repeat(jnp.exp(steps), dims[dim] // parts).reshape((-1,) + (1,) * (len(dims) - 1 - dim))
    return gain


def gaussian(key, extent, deviation, bound, split=(), held_as=jnp.bfloat16):
    drawn = jax.random.normal(key, extent, jnp.float32) * deviation
    if len(split) > 0:
        drawn = block_levels(key, extent, split, -0.22, 0.18) * drawn
    return jnp.clip(drawn, min=-bound, max=bound).astype(held_as)


def setup_inputs(seed: int = 0) -> dict:
    key_list = jax.random.split(jax.random.key(seed), 8)
    observed = jnp.clip(jnp.exp(math.log(8.0) - 3.465736 * jax.random.uniform(key_list[0], (N_DP, N_SECTION, N_TENSOR, LT), jnp.float32) ** block_levels(key_list[0], (N_DP, N_SECTION, N_TENSOR, LT), ((0, 4), (1, 2), (2, 4)), -0.2, 0.2)), 0.25, 8.0)
    section_of = draw_section_of(jax.random.fold_in(key_list[7], 71), 0)
    hist_len = with_ends(jax.random.randint(key_list[2], (NT,), 1, HIST), jax.random.fold_in(key_list[2], 1), 1, HIST - 1).astype(jnp.int32)
    roll_index = jax.random.randint(key_list[3], (), 0, HIST).astype(jnp.int32)
    history = jnp.clip(jnp.exp(jax.random.uniform(key_list[4], (HIST, LT), jnp.float32, math.log(0.02), math.log(64.0))), 0.02, 64.0)
    acts = gaussian(key_list[5], (N_SECTION, TOKENS, D), 1.0, 6.0, ((0, 2), (1, 4), (2, 4)))
    grads = gaussian(key_list[6], (N_SECTION, TOKENS, KV), 1.0, 6.0, ((0, 2), (1, 4), (2, 4)))
    return dict(observed=observed, section_of=section_of, hist_len=hist_len, roll_index=roll_index, history=history, acts=acts, grads=grads)


FP8_MAX = 448.0


def reference(observed, section_of, hist_len, roll_index, history, acts, grads):
    owner = jnp.repeat(section_of, NT)
    sections = jnp.arange(N_SECTION, dtype=jnp.int32).reshape(1, N_SECTION, 1, 1)
    owned = owner.reshape(1, 1, 1, LAYERS * NT) == sections
    merged = jnp.max(jnp.where(owned, observed, jnp.float32(0.0)), axis=(0, 1, 2))
    kind_len = jnp.tile(hist_len, LAYERS)
    slots = jnp.arange(HIST, dtype=jnp.int32).reshape(HIST, 1)
    age = (roll_index - slots) % HIST
    old_window = (age >= 1) & (age <= kind_len[None, :])
    old_scale = FP8_MAX / jnp.max(jnp.where(old_window, history, jnp.float32(0.0)), axis=0)
    new_history = jnp.where(slots == roll_index, merged[None, :], history)
    new_window = age < kind_len[None, :]
    new_scale = FP8_MAX / jnp.max(jnp.where(new_window, new_history, jnp.float32(0.0)), axis=0)
    results = []
    for section in range(N_SECTION):
        first = jnp.sum((section_of < section).astype(jnp.int32))
        scale_x = old_scale[first * NT]
        scale_g = old_scale[first * NT + 1]
        denom = scale_x * scale_g
        acts_q = jnp.clip(acts[section].astype(jnp.float32) * scale_x, -FP8_MAX, FP8_MAX).astype(jnp.bfloat16)
        grads_q = jnp.clip(grads[section].astype(jnp.float32) * scale_g, -FP8_MAX, FP8_MAX).astype(jnp.bfloat16)
        acts_q = acts_q.reshape(N_DP, TOK_DEV, D)
        grads_q = grads_q.reshape(N_DP, TOK_DEV, KV)

        def accumulate(total, pair):
            xpart, gpart = pair
            term = lax.dot_general(xpart, gpart, (((0,), (0,)), ((), ())), preferred_element_type=jnp.float32) / denom
            term = lax.optimization_barrier(term.astype(jnp.bfloat16))
            return total + term.astype(jnp.float32), None

        total, unused = lax.scan(accumulate, jnp.zeros((D, KV), jnp.float32), (acts_q, grads_q))
        results.append(total.astype(jnp.bfloat16))
    return new_history, new_scale, jnp.stack(results)
```

```python
import functools

import jax
import jax.numpy as jnp
from jax import lax
from jax.experimental import pallas as pl
from jax.experimental.pallas import tpu as pltpu
from jax.sharding import PartitionSpec as P

FP8_MAX = 448.0
MESH = pl.DeviceIdType.MESH
LANES = 128


def quantize(values, scale):
    return jnp.clip(values.astype(jnp.float32) * scale, -FP8_MAX, FP8_MAX).astype(jnp.bfloat16)


def kernel(
    ndp, nsec, nt, cw,
    roll_ref, len_ref, sec_ref, obs_ref, hist_ref, acts_ref, grads_ref,
    nh_ref, ns_ref, w_ref,
    abuf, gbuf, gq, acc, obuf, hbuf, hout, pre, mine,
    mxbuf, m1buf, mcbuf, m2buf, mzbuf,
    local_sem, ap_sem, a_send, a_recv, gx_send, gx_recv, gz_send, gz_recv, gc_send, gc_recv,
    mx_send, mx_recv, mc_send, mc_recv, mz_send, mz_recv,
):
    d = lax.axis_index("dp")
    s = lax.axis_index("section")
    t = lax.axis_index("tensor")
    core = lax.rem(d, 2)
    pair = d // 2
    partner = d + 1 - 2 * core
    npair = ndp // 2
    T, cols = acts_ref.shape
    w = cols // ndp
    nq = w // cw
    gw = grads_ref.shape[1]
    slots, LT = hist_ref.shape
    kinds = len_ref.shape[0]

    def dev(dp=None, section=None, tensor=None):
        return {
            "dp": d if dp is None else dp,
            "section": s if section is None else section,
            "tensor": t if tensor is None else tensor,
        }

    other_pairs = [lax.rem(pair + j, npair) for j in range(1, npair)]
    other_t = [lax.rem(t + j, nt) for j in range(1, nt)]
    others_sc = []
    for k in range(nsec):
        for c in range(2):
            if k == 0 and c == 0:
                continue
            sec = lax.rem(s + k, nsec)
            dp = 2 * pair + lax.rem(core + c, 2)
            others_sc.append((sec, dp))

    barrier = pltpu.get_barrier_semaphore()
    count = 0
    for p in other_pairs:
        for c in range(2):
            pl.semaphore_signal(barrier, inc=1, device_id=dev(dp=2 * p + c), device_id_type=MESH)
            count += 1
    for tt in other_t:
        pl.semaphore_signal(barrier, inc=1, device_id=dev(tensor=tt), device_id_type=MESH)
        count += 1
    for sec, dp in others_sc:
        pl.semaphore_signal(
            barrier, inc=1, device_id=dev(dp=dp, section=sec), device_id_type=MESH
        )
        count += 1

    own_rows = pl.ds(pl.multiple_of(d * T, T), T)
    load_hist = pltpu.make_async_copy(hist_ref, hbuf, local_sem.at[0])
    load_hist.start()
    load_acts = pltpu.make_async_copy(
        acts_ref.at[:, pl.ds(pl.multiple_of(d * w, w), w)], abuf.at[own_rows, :], local_sem.at[1]
    )
    load_acts.start()
    load_grads = pltpu.make_async_copy(grads_ref, gbuf.at[t, own_rows, :], local_sem.at[2])
    load_grads.start()

    pl.semaphore_wait(barrier, count)

    sends = []

    def send(src, dst, ssem, rsem, device):
        copy = pltpu.make_async_remote_copy(
            src_ref=src, dst_ref=dst, send_sem=ssem, recv_sem=rsem,
            device_id=device, device_id_type=MESH,
        )
        copy.start()
        sends.append(copy)

    def arrived(dst, ssem, rsem):
        pltpu.make_async_remote_copy(
            src_ref=dst, dst_ref=dst, send_sem=ssem, recv_sem=rsem,
            device_id=dev(dp=partner), device_id_type=MESH,
        ).wait_recv()

    def shard(dp, tt):
        return gbuf.at[tt, pl.ds(pl.multiple_of(dp * T, T), T), :]

    for p in other_pairs:
        send(obs_ref, mxbuf.at[pair], mx_send.at[p], mx_recv.at[pair], dev(dp=2 * p + core))
        send(grads_ref, shard(d, t), gx_send.at[p], gx_recv.at[pair], dev(dp=2 * p + core))
    for tt in other_t:
        send(grads_ref, shard(d, t), gz_send.at[pair, tt], gz_recv.at[pair, t], dev(tensor=tt))
    send(grads_ref, shard(d, t), gc_send.at[pair, t], gc_recv.at[pair, t], dev(dp=partner))
    send(
        acts_ref.at[:, pl.ds(pl.multiple_of(partner * w, w), w)], abuf.at[own_rows, :],
        ap_sem.at[0], ap_sem.at[1], dev(dp=partner),
    )
    for q in range(nq):
        for p in other_pairs:
            for c in range(2):
                dest = 2 * p + c
                send(
                    acts_ref.at[:, pl.ds(pl.multiple_of(dest * w + q * cw, cw), cw)],
                    abuf.at[own_rows, pl.ds(q * cw, cw)],
                    a_send.at[q, dest], a_recv.at[q, d], dev(dp=dest),
                )

    layers = sec_ref[...]
    first = jnp.sum((layers < s).astype(jnp.int32), axis=1, keepdims=True) * kinds
    last = jnp.sum((layers <= s).astype(jnp.int32), axis=1, keepdims=True) * kinds
    column = lax.broadcasted_iota(jnp.int32, (1, LT), 1)
    owned = (column >= first) & (column < last)

    for p in other_pairs:
        arrived(mxbuf.at[p], mx_send.at[p], mx_recv.at[p])
    merged = obs_ref[...]
    for p in other_pairs:
        merged = jnp.maximum(merged, mxbuf[p])
    m1buf[...] = jnp.where(owned, merged, 0.0)
    for k, (sec, dp) in enumerate(others_sc):
        send(
            m1buf, mcbuf.at[2 * s + core], mc_send.at[k], mc_recv.at[2 * s + core],
            dev(dp=dp, section=sec),
        )

    for p in other_pairs:
        e = 2 * p + core
        arrived(shard(e, t), gx_send.at[p], gx_recv.at[p])
        for tt in other_t:
            send(shard(e, t), shard(e, t), gz_send.at[p, tt], gz_recv.at[p, t], dev(tensor=tt))
        send(shard(e, t), shard(e, t), gc_send.at[p, t], gc_recv.at[p, t], dev(dp=partner))

    for sec, dp in others_sc:
        slot = 2 * sec + lax.rem(dp, 2)
        arrived(mcbuf.at[slot], mc_send.at[0], mc_recv.at[slot])
    merged = m1buf[...]
    for sec, dp in others_sc:
        merged = jnp.maximum(merged, mcbuf[2 * sec + lax.rem(dp, 2)])
    m2buf[...] = merged
    for tt in other_t:
        send(m2buf, mzbuf.at[t], mz_send.at[tt], mz_recv.at[t], dev(tensor=tt))

    load_hist.wait()
    roll = roll_ref[0]
    slot_id = lax.broadcasted_iota(jnp.int32, (slots, 1), 0)
    age = roll - slot_id
    age = jnp.where(age < 0, age + slots, age)
    best_x = jnp.zeros((1, 1), jnp.float32)
    best_g = jnp.zeros((1, 1), jnp.float32)
    in_x = (age >= 1) & (age <= len_ref[0])
    in_g = (age >= 1) & (age <= len_ref[1])
    blocks = [(b, min(b + LANES, LT)) for b in range(0, LT, LANES)]
    for lo, hi in blocks:
        h = hbuf[:, lo:hi]
        col = lo + lax.broadcasted_iota(jnp.int32, (1, hi - lo), 1)
        group = jnp.floor((col.astype(jnp.float32) + 0.5) * (1.0 / kinds)).astype(jnp.int32)
        kind = col - group * kinds
        length = jnp.zeros((1, hi - lo), jnp.int32)
        for i in range(kinds):
            length = jnp.where(kind == i, len_ref[i], length)
        window = (age >= 1) & (age < length)
        pre[:, lo:hi] = jnp.max(jnp.where(window, h, 0.0), axis=0, keepdims=True)
        hx = jnp.max(jnp.where(in_x, h, 0.0), axis=0, keepdims=True)
        hg = jnp.max(jnp.where(in_g, h, 0.0), axis=0, keepdims=True)
        best_x = jnp.maximum(
            best_x, jnp.max(jnp.where(col == first, hx, 0.0), axis=1, keepdims=True)
        )
        best_g = jnp.maximum(
            best_g, jnp.max(jnp.where(col == first + 1, hg, 0.0), axis=1, keepdims=True)
        )
    sx = FP8_MAX / best_x
    sg = FP8_MAX / best_g
    inverse = 1.0 / (sx * sg)

    load_grads.wait()
    for p in [pair] + other_pairs:
        e = 2 * p + core
        for tt in other_t:
            arrived(shard(e, tt), gz_send.at[p, tt], gz_recv.at[p, tt])
            send(shard(e, tt), shard(e, tt), gc_send.at[p, tt], gc_recv.at[p, tt], dev(dp=partner))

    for tt in other_t:
        arrived(mzbuf.at[tt], mz_send.at[tt], mz_recv.at[tt])
    merged = m2buf[...]
    for tt in other_t:
        merged = jnp.maximum(merged, mzbuf[tt])
    mine[...] = merged
    ns_ref[...] = FP8_MAX / jnp.maximum(pre[...], merged)
    for lo, hi in blocks:
        hout[:, lo:hi] = jnp.where(slot_id == roll, mine[:, lo:hi], hbuf[:, lo:hi])
    store_hist = pltpu.make_async_copy(hout, nh_ref, local_sem.at[3])
    store_hist.start()

    for p in [pair] + other_pairs:
        for tt in range(nt):
            arrived(shard(2 * p + 1 - core, tt), gc_send.at[p, tt], gc_recv.at[p, tt])

    def rows_of(p):
        return pl.ds(pl.multiple_of(p * 2 * T, 2 * T), 2 * T)

    for p in [pair] + other_pairs:
        for tt in range(nt):
            gq[rows_of(p), tt * gw:(tt + 1) * gw] = quantize(gbuf[tt, rows_of(p), :], sg)

    def product(p, q):
        a = quantize(abuf[rows_of(p), q * cw:(q + 1) * cw], sx)
        return lax.dot_general(
            a, gq[rows_of(p), :], (((0,), (0,)), ((), ())), preferred_element_type=jnp.float32
        )

    load_acts.wait()
    arrived(abuf.at[pl.ds(pl.multiple_of(partner * T, T), T), :], ap_sem.at[0], ap_sem.at[1])
    for q in range(nq):
        acc[q * cw:(q + 1) * cw, :] = product(pair, q)
    stores = []
    for q in range(nq):
        span = slice(q * cw, (q + 1) * cw)
        for j, p in enumerate(other_pairs):
            for c in range(2):
                src = 2 * p + c
                arrived(
                    abuf.at[pl.ds(pl.multiple_of(src * T, T), T), pl.ds(q * cw, cw)],
                    a_send.at[q, src], a_recv.at[q, src],
                )
            acc[span, :] += product(p, q)
        obuf[span, :] = (acc[span, :] * inverse).astype(jnp.bfloat16)
        store = pltpu.make_async_copy(obuf.at[span, :], w_ref.at[span, :], local_sem.at[4 + q])
        store.start()
        stores.append(store)
    store_hist.wait()
    for copy in sends:
        copy.wait_send()
    for store in stores:
        store.wait()


def solution(mesh):
    ndp, nsec, nt = mesh.shape["dp"], mesh.shape["section"], mesh.shape["tensor"]

    def body(observed, section_of, hist_len, roll_index, history, acts, grads):
        slots, LT = history.shape
        T, cols = acts.shape[1:]
        gw = grads.shape[2]
        w = cols // ndp
        cw = min(w, 256)
        nq = w // cw
        npair = ndp // 2
        kv = gw * nt
        f32, bf16 = jnp.float32, jnp.bfloat16
        dma = pltpu.SemaphoreType.DMA
        any_spec = pl.BlockSpec(memory_space=pl.ANY)
        vmem = pl.BlockSpec(memory_space=pltpu.VMEM)
        smem = pl.BlockSpec(memory_space=pltpu.SMEM)
        new_history, new_scale, wgrad = pl.pallas_call(
            functools.partial(kernel, ndp, nsec, nt, cw),
            out_shape=(
                jax.ShapeDtypeStruct((slots, LT), f32),
                jax.ShapeDtypeStruct((1, LT), f32),
                jax.ShapeDtypeStruct((w, kv), bf16),
            ),
            in_specs=[smem, smem, vmem, vmem, any_spec, any_spec, any_spec],
            out_specs=(any_spec, vmem, any_spec),
            scratch_shapes=[
                pltpu.VMEM((ndp * T, w), bf16),
                pltpu.VMEM((nt, ndp * T, gw), bf16),
                pltpu.VMEM((ndp * T, kv), bf16),
                pltpu.VMEM((w, kv), f32),
                pltpu.VMEM((w, kv), bf16),
                pltpu.VMEM((slots, LT), f32),
                pltpu.VMEM((slots, LT), f32),
                pltpu.VMEM((1, LT), f32),
                pltpu.VMEM((1, LT), f32),
                pltpu.VMEM((npair, 1, LT), f32),
                pltpu.VMEM((1, LT), f32),
                pltpu.VMEM((2 * nsec, 1, LT), f32),
                pltpu.VMEM((1, LT), f32),
                pltpu.VMEM((nt, 1, LT), f32),
                dma((4 + nq,)),
                dma((2,)),
                dma((nq, ndp)),
                dma((nq, ndp)),
                dma((npair,)),
                dma((npair,)),
                dma((npair, nt)),
                dma((npair, nt)),
                dma((npair, nt)),
                dma((npair, nt)),
                dma((npair,)),
                dma((npair,)),
                dma((2 * nsec,)),
                dma((2 * nsec,)),
                dma((nt,)),
                dma((nt,)),
            ],
            compiler_params=pltpu.CompilerParams(
                collective_id=0, has_side_effects=True, vmem_limit_bytes=60 * 1024 * 1024
            ),
            name="merge_and_grad",
        )(
            roll_index.reshape(1), hist_len, section_of.reshape(1, -1),
            observed.reshape(1, LT), history, acts[0], grads[0],
        )
        return new_history, new_scale.reshape(LT), wgrad[None]

    in_specs = (
        P("dp", "section", "tensor", None),
        P(),
        P(),
        P(),
        P(),
        P("section", "dp", "tensor"),
        P("section", "dp", "tensor"),
    )
    out_specs = (P(), P(), P("section", ("tensor", "dp"), None))
    return jax.shard_map(body, mesh=mesh, in_specs=in_specs, out_specs=out_specs, check_vma=False)
```

```python
import functools

import jax
import jax.numpy as jnp
from jax import lax
from jax.experimental import pallas as pl
from jax.experimental.pallas import tpu as pltpu
from jax.sharding import PartitionSpec as P

FP8_MAX = 448.0
MESH = pl.DeviceIdType.MESH
LANES = 128


def quantize(values, scale):
    return jnp.clip(values.astype(jnp.float32) * scale, -FP8_MAX, FP8_MAX).astype(jnp.bfloat16)


def kernel(
    ndp, nsec, nt, cw,
    roll_ref, len_ref, sec_ref, obs_ref, hist_ref, acts_ref, grads_ref,
    nh_ref, ns_ref, w_ref,
    abuf, gbuf, gq, acc, obuf, hbuf, hout, pre, mine,
    mxbuf, m1buf, mcbuf, m2buf, mzbuf,
    local_sem, ap_sem, a_send, a_recv, gx_send, gx_recv, gr_send, gl_send, gz_recv, gc_send, gc_recv,
    mx_send, mx_recv, mc_send, mc_recv, mz_send, mz_recv,
):
    d = lax.axis_index("dp")
    s = lax.axis_index("section")
    t = lax.axis_index("tensor")
    core = lax.rem(d, 2)
    pair = d // 2
    partner = d + 1 - 2 * core
    npair = ndp // 2
    T, cols = acts_ref.shape
    w = cols // ndp
    nq = w // cw
    gw = grads_ref.shape[1]
    LT, slots = hist_ref.shape
    kinds = len_ref.shape[0]

    def dev(dp=None, section=None, tensor=None):
        return {
            "dp": d if dp is None else dp,
            "section": s if section is None else section,
            "tensor": t if tensor is None else tensor,
        }

    other_pairs = [lax.rem(pair + j, npair) for j in range(1, npair)]
    other_t = [lax.rem(t + j, nt) for j in range(1, nt)]
    others_sc = []
    for k in range(nsec):
        for c in range(2):
            if k == 0 and c == 0:
                continue
            sec = lax.rem(s + k, nsec)
            dp = 2 * pair + lax.rem(core + c, 2)
            others_sc.append((sec, dp))

    barrier = pltpu.get_barrier_semaphore()
    count = 0
    for p in other_pairs:
        for c in range(2):
            pl.semaphore_signal(barrier, inc=1, device_id=dev(dp=2 * p + c), device_id_type=MESH)
            count += 1
    for tt in other_t:
        pl.semaphore_signal(barrier, inc=1, device_id=dev(tensor=tt), device_id_type=MESH)
        count += 1
    for sec, dp in others_sc:
        pl.semaphore_signal(
            barrier, inc=1, device_id=dev(dp=dp, section=sec), device_id_type=MESH
        )
        count += 1

    own_rows = pl.ds(pl.multiple_of(d * T, T), T)
    load_hist = pltpu.make_async_copy(hist_ref, hbuf.at[pl.ds(0, LT), :], local_sem.at[0])
    load_hist.start()
    load_acts = pltpu.make_async_copy(
        acts_ref.at[:, pl.ds(pl.multiple_of(d * w, w), w)], abuf.at[own_rows, :], local_sem.at[1]
    )
    load_acts.start()
    load_grads = pltpu.make_async_copy(grads_ref, gbuf.at[t, own_rows, :], local_sem.at[2])
    load_grads.start()

    pl.semaphore_wait(barrier, count)

    sends = []

    def send(src, dst, ssem, rsem, device):
        copy = pltpu.make_async_remote_copy(
            src_ref=src, dst_ref=dst, send_sem=ssem, recv_sem=rsem,
            device_id=device, device_id_type=MESH,
        )
        copy.start()
        sends.append(copy)

    def arrived(dst, ssem, rsem):
        pltpu.make_async_remote_copy(
            src_ref=dst, dst_ref=dst, send_sem=ssem, recv_sem=rsem,
            device_id=dev(dp=partner), device_id_type=MESH,
        ).wait_recv()

    def shard(dp, tt):
        return gbuf.at[tt, pl.ds(pl.multiple_of(dp * T, T), T), :]

    for p in other_pairs:
        send(obs_ref, mxbuf.at[pair], mx_send.at[p], mx_recv.at[pair], dev(dp=2 * p + core))
        send(grads_ref, shard(d, t), gx_send.at[p], gx_recv.at[pair], dev(dp=2 * p + core))
    def along(src, p, origin, right):
        here = shard(2 * p + core, origin)
        ssem = (gr_send if right else gl_send).at[p, origin]
        there = t + 1 if right else t - 1
        return pltpu.make_async_remote_copy(
            src_ref=here if src is None else src, dst_ref=here, send_sem=ssem,
            recv_sem=gz_recv.at[p, origin],
            device_id=dev(tensor=there), device_id_type=MESH,
        )

    passed = []

    def pass_on(src, p, origin, right, has_origin):
        cond = has_origin & ((t < nt - 1) if right else (t > 0))
        pl.when(cond)(lambda: along(src, p, origin, right).start())
        passed.append((cond, src, p, origin, right))

    def to_core(p, origin):
        here = shard(2 * p + core, origin)
        return pltpu.make_async_remote_copy(
            src_ref=here, dst_ref=here, send_sem=gc_send.at[p, origin],
            recv_sem=gc_recv.at[p, origin], device_id=dev(dp=partner), device_id_type=MESH,
        )

    def relay(p, k):
        for right in (True, False):
            origin = t - k if right else t + k
            has = (origin >= 0) if right else (origin < nt)

            @pl.when(has)
            def take():
                along(None, p, origin, right).wait_recv()
                to_core(p, origin).start()

            if k < nt - 1:
                pass_on(None, p, origin, right, has)

    always = t >= 0
    pass_on(grads_ref, pair, t, True, always)
    pass_on(grads_ref, pair, t, False, always)
    send(grads_ref, shard(d, t), gc_send.at[pair, t], gc_recv.at[pair, t], dev(dp=partner))
    send(
        acts_ref.at[:, pl.ds(pl.multiple_of(partner * w, w), w)], abuf.at[own_rows, :],
        ap_sem.at[0], ap_sem.at[1], dev(dp=partner),
    )
    for q in range(nq):
        for p in other_pairs:
            for c in range(2):
                dest = 2 * p + c
                send(
                    acts_ref.at[:, pl.ds(pl.multiple_of(dest * w + q * cw, cw), cw)],
                    abuf.at[own_rows, pl.ds(q * cw, cw)],
                    a_send.at[q, dest], a_recv.at[q, d], dev(dp=dest),
                )

    layers = sec_ref[...]
    first = jnp.sum((layers < s).astype(jnp.int32), axis=1, keepdims=True) * kinds
    last = jnp.sum((layers <= s).astype(jnp.int32), axis=1, keepdims=True) * kinds
    column = lax.broadcasted_iota(jnp.int32, (1, LT), 1)
    owned = (column >= first) & (column < last)

    for p in other_pairs:
        arrived(mxbuf.at[p], mx_send.at[p], mx_recv.at[p])
    merged = obs_ref[...]
    for p in other_pairs:
        merged = jnp.maximum(merged, mxbuf[p])
    m1buf[...] = jnp.where(owned, merged, 0.0)
    for k, (sec, dp) in enumerate(others_sc):
        send(
            m1buf, mcbuf.at[2 * s + core], mc_send.at[k], mc_recv.at[2 * s + core],
            dev(dp=dp, section=sec),
        )

    def from_other_pairs(k):
        for p in other_pairs:
            if k == 0:
                e = 2 * p + core
                arrived(shard(e, t), gx_send.at[p], gx_recv.at[p])
                pass_on(None, p, t, True, always)
                pass_on(None, p, t, False, always)
                send(shard(e, t), shard(e, t), gc_send.at[p, t], gc_recv.at[p, t], dev(dp=partner))
            else:
                relay(p, k)

    for sec, dp in others_sc:
        slot = 2 * sec + lax.rem(dp, 2)
        arrived(mcbuf.at[slot], mc_send.at[0], mc_recv.at[slot])
    merged = m1buf[...]
    for sec, dp in others_sc:
        merged = jnp.maximum(merged, mcbuf[2 * sec + lax.rem(dp, 2)])
    m2buf[...] = merged
    for tt in other_t:
        send(m2buf, mzbuf.at[t], mz_send.at[tt], mz_recv.at[t], dev(tensor=tt))

    load_hist.wait()
    roll = roll_ref[0]
    slot_id = lax.broadcasted_iota(jnp.int32, (slots, 1), 0)
    lane_id = lax.broadcasted_iota(jnp.int32, (1, slots), 1)
    age = roll - slot_id
    age = jnp.where(age < 0, age + slots, age)
    best_x = jnp.zeros((1, 1), jnp.float32)
    best_g = jnp.zeros((1, 1), jnp.float32)
    in_x = (age >= 1) & (age <= len_ref[0])
    in_g = (age >= 1) & (age <= len_ref[1])
    blocks = [(b, b + LANES) for b in range(0, LT, LANES)]
    for lo, hi in blocks:
        h = hbuf[lo:hi, :].T
        col = lo + lax.broadcasted_iota(jnp.int32, (1, hi - lo), 1)
        group = jnp.floor((col.astype(jnp.float32) + 0.5) * (1.0 / kinds)).astype(jnp.int32)
        kind = col - group * kinds
        length = jnp.zeros((1, hi - lo), jnp.int32)
        for i in range(kinds):
            length = jnp.where(kind == i, len_ref[i], length)
        window = (age >= 1) & (age < length)
        pre[:, lo:hi] = jnp.max(jnp.where(window, h, 0.0), axis=0, keepdims=True)
        hx = jnp.max(jnp.where(in_x, h, 0.0), axis=0, keepdims=True)
        hg = jnp.max(jnp.where(in_g, h, 0.0), axis=0, keepdims=True)
        best_x = jnp.maximum(
            best_x, jnp.max(jnp.where(col == first, hx, 0.0), axis=1, keepdims=True)
        )
        best_g = jnp.maximum(
            best_g, jnp.max(jnp.where(col == first + 1, hg, 0.0), axis=1, keepdims=True)
        )
    sx = FP8_MAX / best_x
    sg = FP8_MAX / best_g
    inverse = 1.0 / (sx * sg)

    load_grads.wait()
    for k in range(1, nt):
        relay(pair, k)
        if k < nt:
            from_other_pairs(k - 1)

    for tt in other_t:
        arrived(mzbuf.at[tt], mz_send.at[tt], mz_recv.at[tt])
    merged = m2buf[...]
    for tt in other_t:
        merged = jnp.maximum(merged, mzbuf[tt])
    mine[:, 0:LT] = merged
    ns_ref[...] = FP8_MAX / jnp.maximum(pre[:, 0:LT], merged)
    for lo, hi in blocks:
        row = jnp.broadcast_to(mine[:, lo:hi], (slots, hi - lo)).T
        hout[lo:hi, :] = jnp.where(lane_id == roll, row, hbuf[lo:hi, :])
    store_hist = pltpu.make_async_copy(hout.at[pl.ds(0, LT), :], nh_ref, local_sem.at[3])
    store_hist.start()

    def rows_of(p):
        return pl.ds(pl.multiple_of(p * 2 * T, 2 * T), 2 * T)

    def grads_of(p):
        for tt in range(nt):
            arrived(shard(2 * p + 1 - core, tt), gc_send.at[p, tt], gc_recv.at[p, tt])
        for tt in range(nt):
            gq[rows_of(p), tt * gw:(tt + 1) * gw] = quantize(gbuf[tt, rows_of(p), :], sg)

    def product(p, q):
        a = quantize(abuf[rows_of(p), q * cw:(q + 1) * cw], sx)
        return lax.dot_general(
            a, gq[rows_of(p), :], (((0,), (0,)), ((), ())), preferred_element_type=jnp.float32
        )

    load_acts.wait()
    arrived(abuf.at[pl.ds(pl.multiple_of(partner * T, T), T), :], ap_sem.at[0], ap_sem.at[1])
    grads_of(pair)
    for q in range(nq):
        acc[q * cw:(q + 1) * cw, :] = product(pair, q)
    from_other_pairs(nt - 1)
    for p in other_pairs:
        grads_of(p)
    stores = []
    for q in range(nq):
        span = slice(q * cw, (q + 1) * cw)
        for j, p in enumerate(other_pairs):
            for c in range(2):
                src = 2 * p + c
                arrived(
                    abuf.at[pl.ds(pl.multiple_of(src * T, T), T), pl.ds(q * cw, cw)],
                    a_send.at[q, src], a_recv.at[q, src],
                )
            acc[span, :] += product(p, q)
        obuf[span, :] = (acc[span, :] * inverse).astype(jnp.bfloat16)
        store = pltpu.make_async_copy(obuf.at[span, :], w_ref.at[span, :], local_sem.at[4 + q])
        store.start()
        stores.append(store)
    store_hist.wait()
    for copy in sends:
        copy.wait_send()
    for cond, src, p, origin, right in passed:
        pl.when(cond)(lambda: along(src, p, origin, right).wait_send())
    for p in [pair] + other_pairs:
        for k in range(1, nt):
            for origin, has in ((t - k, t - k >= 0), (t + k, t + k < nt)):
                pl.when(has)(lambda: to_core(p, origin).wait_send())
    for store in stores:
        store.wait()


def solution(mesh):
    ndp, nsec, nt = mesh.shape["dp"], mesh.shape["section"], mesh.shape["tensor"]

    def body(observed, section_of, hist_len, roll_index, history, acts, grads):
        slots, LT = history.shape
        T, cols = acts.shape[1:]
        gw = grads.shape[2]
        w = cols // ndp
        cw = min(w, 256)
        nq = w // cw
        npair = ndp // 2
        kv = gw * nt
        padded = pl.cdiv(LT, LANES) * LANES
        f32, bf16 = jnp.float32, jnp.bfloat16
        dma = pltpu.SemaphoreType.DMA
        hbm = pl.BlockSpec(memory_space=pltpu.HBM)
        any_spec = pl.BlockSpec(memory_space=pl.ANY)
        vmem = pl.BlockSpec(memory_space=pltpu.VMEM)
        smem = pl.BlockSpec(memory_space=pltpu.SMEM)
        new_history, new_scale, wgrad = pl.pallas_call(
            functools.partial(kernel, ndp, nsec, nt, cw),
            out_shape=(
                jax.ShapeDtypeStruct((LT, slots), f32),
                jax.ShapeDtypeStruct((1, LT), f32),
                jax.ShapeDtypeStruct((w, kv), bf16),
            ),
            in_specs=[smem, smem, vmem, vmem, hbm, hbm, hbm],
            out_specs=(any_spec, vmem, any_spec),
            scratch_shapes=[
                pltpu.VMEM((ndp * T, w), bf16),
                pltpu.VMEM((nt, ndp * T, gw), bf16),
                pltpu.VMEM((ndp * T, kv), bf16),
                pltpu.VMEM((w, kv), f32),
                pltpu.VMEM((w, kv), bf16),
                pltpu.VMEM((padded, slots), f32),
                pltpu.VMEM((padded, slots), f32),
                pltpu.VMEM((1, padded), f32),
                pltpu.VMEM((1, padded), f32),
                pltpu.VMEM((npair, 1, LT), f32),
                pltpu.VMEM((1, LT), f32),
                pltpu.VMEM((2 * nsec, 1, LT), f32),
                pltpu.VMEM((1, LT), f32),
                pltpu.VMEM((nt, 1, LT), f32),
                dma((4 + nq,)),
                dma((2,)),
                dma((nq, ndp)),
                dma((nq, ndp)),
                dma((npair,)),
                dma((npair,)),
                dma((npair, nt)),
                dma((npair, nt)),
                dma((npair, nt)),
                dma((npair, nt)),
                dma((npair, nt)),
                dma((npair,)),
                dma((npair,)),
                dma((2 * nsec,)),
                dma((2 * nsec,)),
                dma((nt,)),
                dma((nt,)),
            ],
            compiler_params=pltpu.CompilerParams(
                collective_id=0, has_side_effects=True, vmem_limit_bytes=60 * 1024 * 1024
            ),
            name="merge_and_grad",
        )(
            roll_index.reshape(1), hist_len, section_of.reshape(1, -1),
            observed.reshape(1, LT), history.T, acts[0], grads[0],
        )
        return new_history.T, new_scale.reshape(LT), wgrad[None]

    in_specs = (
        P("dp", "section", "tensor", None),
        P(),
        P(),
        P(),
        P(),
        P("section", "dp", "tensor"),
        P("section", "dp", "tensor"),
    )
    out_specs = (P(), P(), P("section", ("tensor", "dp"), None))
    return jax.shard_map(body, mesh=mesh, in_specs=in_specs, out_specs=out_specs, check_vma=False)
```

```python
import functools

import jax
import jax.numpy as jnp
from jax import lax
from jax.experimental import pallas as pl
from jax.experimental.pallas import tpu as pltpu
from jax.sharding import PartitionSpec as P

FP8_MAX = 448.0
MESH = pl.DeviceIdType.MESH
LANES = 128


def quantize(values, scale):
    return jnp.clip(values.astype(jnp.float32) * scale, -FP8_MAX, FP8_MAX).astype(jnp.bfloat16)


def kernel(
    ndp, nsec, nt, cw,
    roll_ref, len_ref, sec_ref, obs_ref, hist_ref, acts_ref, grads_ref,
    nh_ref, ns_ref, w_ref,
    abuf, gbuf, gq, acc, obuf, hbuf, hout, pre, mine,
    mxbuf, m1buf, mcbuf, m2buf, mzbuf,
    local_sem, ap_sem, a_send, a_recv, gx_send, gx_recv, gr_send, gl_send, gz_recv, gc_send, gc_recv,
    mx_send, mx_recv, mc_send, mc_recv, mz_send, mz_recv,
):
    d = lax.axis_index("dp")
    s = lax.axis_index("section")
    t = lax.axis_index("tensor")
    core = lax.rem(d, 2)
    pair = d // 2
    partner = d + 1 - 2 * core
    npair = ndp // 2
    T, cols = acts_ref.shape
    w = cols // ndp
    nq = w // cw
    gw = grads_ref.shape[1]
    LT, slots = hist_ref.shape
    kinds = len_ref.shape[0]

    def dev(dp=None, section=None, tensor=None):
        return {
            "dp": d if dp is None else dp,
            "section": s if section is None else section,
            "tensor": t if tensor is None else tensor,
        }

    other_pairs = [lax.rem(pair + j, npair) for j in range(1, npair)]
    other_t = [lax.rem(t + j, nt) for j in range(1, nt)]
    others_sc = []
    for k in range(nsec):
        for c in range(2):
            if k == 0 and c == 0:
                continue
            sec = lax.rem(s + k, nsec)
            dp = 2 * pair + lax.rem(core + c, 2)
            others_sc.append((sec, dp))

    barrier = pltpu.get_barrier_semaphore()
    count = 0
    for p in other_pairs:
        for c in range(2):
            pl.semaphore_signal(barrier, inc=1, device_id=dev(dp=2 * p + c), device_id_type=MESH)
            count += 1
    for tt in other_t:
        pl.semaphore_signal(barrier, inc=1, device_id=dev(tensor=tt), device_id_type=MESH)
        count += 1
    for sec, dp in others_sc:
        pl.semaphore_signal(
            barrier, inc=1, device_id=dev(dp=dp, section=sec), device_id_type=MESH
        )
        count += 1

    own_rows = pl.ds(pl.multiple_of(d * T, T), T)
    load_hist = pltpu.make_async_copy(hist_ref, hbuf.at[pl.ds(0, LT), :], local_sem.at[0])
    load_hist.start()
    load_acts = pltpu.make_async_copy(
        acts_ref.at[:, pl.ds(pl.multiple_of(d * w, w), w)], abuf.at[own_rows, :], local_sem.at[1]
    )
    load_acts.start()
    load_grads = pltpu.make_async_copy(grads_ref, gbuf.at[t, own_rows, :], local_sem.at[2])
    load_grads.start()

    pl.semaphore_wait(barrier, count)

    sends = []

    def send(src, dst, ssem, rsem, device):
        copy = pltpu.make_async_remote_copy(
            src_ref=src, dst_ref=dst, send_sem=ssem, recv_sem=rsem,
            device_id=device, device_id_type=MESH,
        )
        copy.start()
        sends.append(copy)

    def arrived(dst, ssem, rsem):
        pltpu.make_async_remote_copy(
            src_ref=dst, dst_ref=dst, send_sem=ssem, recv_sem=rsem,
            device_id=dev(dp=partner), device_id_type=MESH,
        ).wait_recv()

    def shard(dp, tt):
        return gbuf.at[tt, pl.ds(pl.multiple_of(dp * T, T), T), :]

    for p in other_pairs:
        send(obs_ref, mxbuf.at[pair], mx_send.at[p], mx_recv.at[pair], dev(dp=2 * p + core))
        send(grads_ref, shard(d, t), gx_send.at[p], gx_recv.at[pair], dev(dp=2 * p + core))
    def along(src, p, origin, right):
        here = shard(2 * p + core, origin)
        ssem = (gr_send if right else gl_send).at[p, origin]
        there = t + 1 if right else t - 1
        return pltpu.make_async_remote_copy(
            src_ref=here if src is None else src, dst_ref=here, send_sem=ssem,
            recv_sem=gz_recv.at[p, origin],
            device_id=dev(tensor=there), device_id_type=MESH,
        )

    passed = []

    def pass_on(src, p, origin, right, has_origin):
        cond = has_origin & ((t < nt - 1) if right else (t > 0))
        pl.when(cond)(lambda: along(src, p, origin, right).start())
        passed.append((cond, src, p, origin, right))

    def to_core(p, origin):
        here = shard(2 * p + core, origin)
        return pltpu.make_async_remote_copy(
            src_ref=here, dst_ref=here, send_sem=gc_send.at[p, origin],
            recv_sem=gc_recv.at[p, origin], device_id=dev(dp=partner), device_id_type=MESH,
        )

    def relay(p, k):
        for right in (True, False):
            origin = t - k if right else t + k
            has = (origin >= 0) if right else (origin < nt)

            @pl.when(has)
            def take():
                along(None, p, origin, right).wait_recv()
                to_core(p, origin).start()

            if k < nt - 1:
                pass_on(None, p, origin, right, has)

    always = t >= 0
    pass_on(grads_ref, pair, t, True, always)
    pass_on(grads_ref, pair, t, False, always)
    send(grads_ref, shard(d, t), gc_send.at[pair, t], gc_recv.at[pair, t], dev(dp=partner))
    send(
        acts_ref.at[:, pl.ds(pl.multiple_of(partner * w, w), w)], abuf.at[own_rows, :],
        ap_sem.at[0], ap_sem.at[1], dev(dp=partner),
    )
    for q in range(nq):
        for p in other_pairs:
            for c in range(2):
                dest = 2 * p + c
                send(
                    acts_ref.at[:, pl.ds(pl.multiple_of(dest * w + q * cw, cw), cw)],
                    abuf.at[own_rows, pl.ds(q * cw, cw)],
                    a_send.at[q, dest], a_recv.at[q, d], dev(dp=dest),
                )

    layers = sec_ref[...]
    first = jnp.sum((layers < s).astype(jnp.int32), axis=1, keepdims=True) * kinds
    last = jnp.sum((layers <= s).astype(jnp.int32), axis=1, keepdims=True) * kinds
    column = lax.broadcasted_iota(jnp.int32, (1, LT), 1)
    owned = (column >= first) & (column < last)

    for p in other_pairs:
        arrived(mxbuf.at[p], mx_send.at[p], mx_recv.at[p])
    merged = obs_ref[...]
    for p in other_pairs:
        merged = jnp.maximum(merged, mxbuf[p])
    m1buf[...] = jnp.where(owned, merged, 0.0)
    for k, (sec, dp) in enumerate(others_sc):
        send(
            m1buf, mcbuf.at[2 * s + core], mc_send.at[k], mc_recv.at[2 * s + core],
            dev(dp=dp, section=sec),
        )

    def from_other_pairs(k):
        for p in other_pairs:
            if k == 0:
                e = 2 * p + core
                arrived(shard(e, t), gx_send.at[p], gx_recv.at[p])
                pass_on(None, p, t, True, always)
                pass_on(None, p, t, False, always)
                send(shard(e, t), shard(e, t), gc_send.at[p, t], gc_recv.at[p, t], dev(dp=partner))
            else:
                relay(p, k)

    for sec, dp in others_sc:
        slot = 2 * sec + lax.rem(dp, 2)
        arrived(mcbuf.at[slot], mc_send.at[0], mc_recv.at[slot])
    merged = m1buf[...]
    for sec, dp in others_sc:
        merged = jnp.maximum(merged, mcbuf[2 * sec + lax.rem(dp, 2)])
    m2buf[...] = merged
    for tt in other_t:
        send(m2buf, mzbuf.at[t], mz_send.at[tt], mz_recv.at[t], dev(tensor=tt))

    load_hist.wait()
    roll = roll_ref[0]
    slot_id = lax.broadcasted_iota(jnp.int32, (slots, 1), 0)
    lane_id = lax.broadcasted_iota(jnp.int32, (1, slots), 1)
    age = roll - slot_id
    age = jnp.where(age < 0, age + slots, age)
    best_x = jnp.zeros((1, 1), jnp.float32)
    best_g = jnp.zeros((1, 1), jnp.float32)
    in_x = (age >= 1) & (age <= len_ref[0])
    in_g = (age >= 1) & (age <= len_ref[1])
    blocks = [(b, b + LANES) for b in range(0, LT, LANES)]
    for lo, hi in blocks:
        h = hbuf[lo:hi, :].T
        col = lo + lax.broadcasted_iota(jnp.int32, (1, hi - lo), 1)
        group = jnp.floor((col.astype(jnp.float32) + 0.5) * (1.0 / kinds)).astype(jnp.int32)
        kind = col - group * kinds
        length = jnp.zeros((1, hi - lo), jnp.int32)
        for i in range(kinds):
            length = jnp.where(kind == i, len_ref[i], length)
        window = (age >= 1) & (age < length)
        pre[:, lo:hi] = jnp.max(jnp.where(window, h, 0.0), axis=0, keepdims=True)
        hx = jnp.max(jnp.where(in_x, h, 0.0), axis=0, keepdims=True)
        hg = jnp.max(jnp.where(in_g, h, 0.0), axis=0, keepdims=True)
        best_x = jnp.maximum(
            best_x, jnp.max(jnp.where(col == first, hx, 0.0), axis=1, keepdims=True)
        )
        best_g = jnp.maximum(
            best_g, jnp.max(jnp.where(col == first + 1, hg, 0.0), axis=1, keepdims=True)
        )
    sx = FP8_MAX / best_x
    sg = FP8_MAX / best_g
    inverse = 1.0 / (sx * sg)

    load_grads.wait()
    for k in range(1, nt):
        relay(pair, k)
        if k < nt:
            from_other_pairs(k - 1)

    for tt in other_t:
        arrived(mzbuf.at[tt], mz_send.at[tt], mz_recv.at[tt])
    merged = m2buf[...]
    for tt in other_t:
        merged = jnp.maximum(merged, mzbuf[tt])
    mine[:, 0:LT] = merged
    ns_ref[...] = FP8_MAX / jnp.maximum(pre[:, 0:LT], merged)
    for lo, hi in blocks:
        row = jnp.broadcast_to(mine[:, lo:hi], (slots, hi - lo)).T
        hout[lo:hi, :] = jnp.where(lane_id == roll, row, hbuf[lo:hi, :])
    store_hist = pltpu.make_async_copy(hout.at[pl.ds(0, LT), :], nh_ref, local_sem.at[3])
    store_hist.start()

    def rows_of(p):
        return pl.ds(pl.multiple_of(p * 2 * T, 2 * T), 2 * T)

    def grads_of(p):
        for tt in range(nt):
            arrived(shard(2 * p + 1 - core, tt), gc_send.at[p, tt], gc_recv.at[p, tt])
        for tt in range(nt):
            gq[rows_of(p), tt * gw:(tt + 1) * gw] = quantize(gbuf[tt, rows_of(p), :], sg)

    def product(p, q):
        a = quantize(abuf[rows_of(p), q * cw:(q + 1) * cw], sx)
        return lax.dot_general(
            a, gq[rows_of(p), :], (((0,), (0,)), ((), ())), preferred_element_type=jnp.float32
        )

    load_acts.wait()
    arrived(abuf.at[pl.ds(pl.multiple_of(partner * T, T), T), :], ap_sem.at[0], ap_sem.at[1])
    grads_of(pair)
    for q in range(nq):
        acc[q * cw:(q + 1) * cw, :] = product(pair, q)
    from_other_pairs(nt - 1)
    for p in other_pairs:
        grads_of(p)
    stores = []
    for q in range(nq):
        span = slice(q * cw, (q + 1) * cw)
        for j, p in enumerate(other_pairs):
            for c in range(2):
                src = 2 * p + c
                arrived(
                    abuf.at[pl.ds(pl.multiple_of(src * T, T), T), pl.ds(q * cw, cw)],
                    a_send.at[q, src], a_recv.at[q, src],
                )
            acc[span, :] += product(p, q)
        obuf[span, :] = (acc[span, :] * inverse).astype(jnp.bfloat16)
        store = pltpu.make_async_copy(obuf.at[span, :], w_ref.at[span, :], local_sem.at[4 + q])
        store.start()
        stores.append(store)
    store_hist.wait()
    for copy in sends:
        copy.wait_send()
    for cond, src, p, origin, right in passed:
        pl.when(cond)(lambda: along(src, p, origin, right).wait_send())
    for p in [pair] + other_pairs:
        for k in range(1, nt):
            for origin, has in ((t - k, t - k >= 0), (t + k, t + k < nt)):
                pl.when(has)(lambda: to_core(p, origin).wait_send())
    for store in stores:
        store.wait()


def hand_over(scale_ref, hist_ref, w_ref, ns_ref, nh_ref, wout_ref, hbuf, wbuf, in_sem, out_sem):
    rows, cut = w_ref.shape[0], hist_ref.shape[0] // 16 * 8
    step = max(rows // 4, 16)
    spans = [(w_ref, wbuf, wout_ref, lo, step) for lo in range(0, rows, step)]
    spans.append((hist_ref, hbuf, nh_ref, 0, cut))
    spans.append((hist_ref, hbuf, nh_ref, cut, hist_ref.shape[0] - cut))
    reads, writes = [], []
    for i, (src, held, dst, lo, n) in enumerate(spans):
        span = pl.ds(lo, n)
        reads.append(pltpu.make_async_copy(src.at[span, :], held.at[span, :], in_sem.at[i]))
        writes.append(pltpu.make_async_copy(held.at[span, :], dst.at[span, :], out_sem.at[i]))
    for read in reads:
        read.start()
    ns_ref[...] = scale_ref[...].reshape(ns_ref.shape)
    for read, write in zip(reads, writes):
        read.wait()
        write.start()
    for write in writes:
        write.wait()


def solution(mesh):
    ndp, nsec, nt = mesh.shape["dp"], mesh.shape["section"], mesh.shape["tensor"]

    def body(observed, section_of, hist_len, roll_index, history, acts, grads):
        slots, LT = history.shape
        T, cols = acts.shape[1:]
        gw = grads.shape[2]
        w = cols // ndp
        cw = min(w, 256)
        nq = w // cw
        npair = ndp // 2
        kv = gw * nt
        padded = pl.cdiv(LT, LANES) * LANES
        f32, bf16 = jnp.float32, jnp.bfloat16
        dma = pltpu.SemaphoreType.DMA
        hbm = pl.BlockSpec(memory_space=pltpu.HBM)
        any_spec = pl.BlockSpec(memory_space=pl.ANY)
        vmem = pl.BlockSpec(memory_space=pltpu.VMEM)
        smem = pl.BlockSpec(memory_space=pltpu.SMEM)
        new_history, new_scale, wgrad = pl.pallas_call(
            functools.partial(kernel, ndp, nsec, nt, cw),
            out_shape=(
                jax.ShapeDtypeStruct((LT, slots), f32),
                jax.ShapeDtypeStruct((1, LT), f32),
                jax.ShapeDtypeStruct((w, kv), bf16),
            ),
            in_specs=[smem, smem, vmem, vmem, hbm, hbm, hbm],
            out_specs=(any_spec, vmem, any_spec),
            scratch_shapes=[
                pltpu.VMEM((ndp * T, w), bf16),
                pltpu.VMEM((nt, ndp * T, gw), bf16),
                pltpu.VMEM((ndp * T, kv), bf16),
                pltpu.VMEM((w, kv), f32),
                pltpu.VMEM((w, kv), bf16),
                pltpu.VMEM((padded, slots), f32),
                pltpu.VMEM((padded, slots), f32),
                pltpu.VMEM((1, padded), f32),
                pltpu.VMEM((1, padded), f32),
                pltpu.VMEM((npair, 1, LT), f32),
                pltpu.VMEM((1, LT), f32),
                pltpu.VMEM((2 * nsec, 1, LT), f32),
                pltpu.VMEM((1, LT), f32),
                pltpu.VMEM((nt, 1, LT), f32),
                dma((4 + nq,)),
                dma((2,)),
                dma((nq, ndp)),
                dma((nq, ndp)),
                dma((npair,)),
                dma((npair,)),
                dma((npair, nt)),
                dma((npair, nt)),
                dma((npair, nt)),
                dma((npair, nt)),
                dma((npair, nt)),
                dma((npair,)),
                dma((npair,)),
                dma((2 * nsec,)),
                dma((2 * nsec,)),
                dma((nt,)),
                dma((nt,)),
            ],
            compiler_params=pltpu.CompilerParams(
                collective_id=0, has_side_effects=True, vmem_limit_bytes=60 * 1024 * 1024
            ),
            name="merge_and_grad",
        )(
            roll_index.reshape(1), hist_len, section_of.reshape(1, -1),
            observed.reshape(1, LT), history.T, acts[0], grads[0],
        )
        new_scale, new_history, wgrad = pl.pallas_call(
            hand_over,
            out_shape=(
                jax.ShapeDtypeStruct((LT,), f32),
                jax.ShapeDtypeStruct((LT, slots), f32),
                jax.ShapeDtypeStruct((w, kv), bf16),
            ),
            in_specs=[vmem, any_spec, any_spec],
            out_specs=(vmem, any_spec, any_spec),
            scratch_shapes=[
                pltpu.VMEM((LT, slots), f32),
                pltpu.VMEM((w, kv), bf16),
                dma((8,)),
                dma((8,)),
            ],
            compiler_params=pltpu.CompilerParams(vmem_limit_bytes=60 * 1024 * 1024),
            name="hand_over",
        )(new_scale, new_history, wgrad)
        return new_history.T, new_scale, wgrad[None]

    in_specs = (
        P("dp", "section", "tensor", None),
        P(),
        P(),
        P(),
        P(),
        P("section", "dp", "tensor"),
        P("section", "dp", "tensor"),
    )
    out_specs = (P(), P(), P("section", ("tensor", "dp"), None))
    return jax.shard_map(body, mesh=mesh, in_specs=in_specs, out_specs=out_specs, check_vma=False)
```

```python
import functools

import jax
import jax.numpy as jnp
from jax import lax
from jax.experimental import pallas as pl
from jax.experimental.pallas import tpu as pltpu
from jax.sharding import PartitionSpec as P

FP8_MAX = 448.0
MESH = pl.DeviceIdType.MESH
LANES = 128


def quantize(values, scale):
    return jnp.clip(values.astype(jnp.float32) * scale, -FP8_MAX, FP8_MAX).astype(jnp.bfloat16)


def chunks(w, cw):
    spans = [(lo, cw) for lo in range(0, w, cw)]
    if cw % (2 * LANES) == 0:
        spans[-1:] = [(w - cw, cw // 2), (w - cw // 2, cw // 2)]
    return spans


def kernel(
    ndp, nsec, nt, cw,
    roll_ref, len_ref, sec_ref, obs_ref, hist_ref, acts_ref, grads_ref,
    nh_ref, ns_ref, w_ref,
    abuf, gbuf, gq, acc, obuf, hbuf, hout, pre, mine,
    mxbuf, m1buf, mcbuf, m2buf, mzbuf,
    local_sem, ap_sem, a_send, a_recv, gx_send, gx_recv, gr_send, gl_send, gz_recv, gc_send, gc_recv,
    mx_send, mx_recv, mc_send, mc_recv, mz_send, mz_recv,
):
    d = lax.axis_index("dp")
    s = lax.axis_index("section")
    t = lax.axis_index("tensor")
    core = lax.rem(d, 2)
    pair = d // 2
    partner = d + 1 - 2 * core
    npair = ndp // 2
    T, cols = acts_ref.shape
    w = cols // ndp
    spans = chunks(w, cw)
    gw = grads_ref.shape[1]
    LT, slots = hist_ref.shape
    kinds = len_ref.shape[0]

    def dev(dp=None, section=None, tensor=None):
        return {
            "dp": d if dp is None else dp,
            "section": s if section is None else section,
            "tensor": t if tensor is None else tensor,
        }

    other_pairs = [lax.rem(pair + j, npair) for j in range(1, npair)]
    other_t = [lax.rem(t + j, nt) for j in range(1, nt)]
    others_sc = []
    for k in range(nsec):
        for c in range(2):
            if k == 0 and c == 0:
                continue
            sec = lax.rem(s + k, nsec)
            dp = 2 * pair + lax.rem(core + c, 2)
            others_sc.append((sec, dp))

    barrier = pltpu.get_barrier_semaphore()
    count = 0
    for p in other_pairs:
        for c in range(2):
            pl.semaphore_signal(barrier, inc=1, device_id=dev(dp=2 * p + c), device_id_type=MESH)
            count += 1
    for tt in other_t:
        pl.semaphore_signal(barrier, inc=1, device_id=dev(tensor=tt), device_id_type=MESH)
        count += 1
    for sec, dp in others_sc:
        pl.semaphore_signal(
            barrier, inc=1, device_id=dev(dp=dp, section=sec), device_id_type=MESH
        )
        count += 1

    own_rows = pl.ds(pl.multiple_of(d * T, T), T)
    load_hist = pltpu.make_async_copy(hist_ref, hbuf.at[pl.ds(0, LT), :], local_sem.at[0])
    load_hist.start()
    load_acts = pltpu.make_async_copy(
        acts_ref.at[:, pl.ds(pl.multiple_of(d * w, w), w)], abuf.at[own_rows, :], local_sem.at[1]
    )
    load_acts.start()
    load_grads = pltpu.make_async_copy(grads_ref, gbuf.at[t, own_rows, :], local_sem.at[2])
    load_grads.start()

    pl.semaphore_wait(barrier, count)

    sends = []

    def send(src, dst, ssem, rsem, device):
        copy = pltpu.make_async_remote_copy(
            src_ref=src, dst_ref=dst, send_sem=ssem, recv_sem=rsem,
            device_id=device, device_id_type=MESH,
        )
        copy.start()
        sends.append(copy)

    def arrived(dst, ssem, rsem):
        pltpu.make_async_remote_copy(
            src_ref=dst, dst_ref=dst, send_sem=ssem, recv_sem=rsem,
            device_id=dev(dp=partner), device_id_type=MESH,
        ).wait_recv()

    def shard(dp, tt):
        return gbuf.at[tt, pl.ds(pl.multiple_of(dp * T, T), T), :]

    for p in other_pairs:
        send(obs_ref, mxbuf.at[pair], mx_send.at[p], mx_recv.at[pair], dev(dp=2 * p + core))
        send(grads_ref, shard(d, t), gx_send.at[p], gx_recv.at[pair], dev(dp=2 * p + core))
    def along(src, p, origin, right):
        here = shard(2 * p + core, origin)
        ssem = (gr_send if right else gl_send).at[p, origin]
        there = t + 1 if right else t - 1
        return pltpu.make_async_remote_copy(
            src_ref=here if src is None else src, dst_ref=here, send_sem=ssem,
            recv_sem=gz_recv.at[p, origin],
            device_id=dev(tensor=there), device_id_type=MESH,
        )

    passed = []

    def pass_on(src, p, origin, right, has_origin):
        cond = has_origin & ((t < nt - 1) if right else (t > 0))
        pl.when(cond)(lambda: along(src, p, origin, right).start())
        passed.append((cond, src, p, origin, right))

    def to_core(p, origin):
        here = shard(2 * p + core, origin)
        return pltpu.make_async_remote_copy(
            src_ref=here, dst_ref=here, send_sem=gc_send.at[p, origin],
            recv_sem=gc_recv.at[p, origin], device_id=dev(dp=partner), device_id_type=MESH,
        )

    def relay(p, k):
        for right in (True, False):
            origin = t - k if right else t + k
            has = (origin >= 0) if right else (origin < nt)

            @pl.when(has)
            def take():
                along(None, p, origin, right).wait_recv()
                to_core(p, origin).start()

            if k < nt - 1:
                pass_on(None, p, origin, right, has)

    always = t >= 0
    pass_on(grads_ref, pair, t, True, always)
    pass_on(grads_ref, pair, t, False, always)
    send(grads_ref, shard(d, t), gc_send.at[pair, t], gc_recv.at[pair, t], dev(dp=partner))
    send(
        acts_ref.at[:, pl.ds(pl.multiple_of(partner * w, w), w)], abuf.at[own_rows, :],
        ap_sem.at[0], ap_sem.at[1], dev(dp=partner),
    )
    for q, (lo, n) in enumerate(spans):
        for p in other_pairs:
            for c in range(2):
                dest = 2 * p + c
                send(
                    acts_ref.at[:, pl.ds(pl.multiple_of(dest * w + lo, LANES), n)],
                    abuf.at[own_rows, pl.ds(lo, n)],
                    a_send.at[q, dest], a_recv.at[q, d], dev(dp=dest),
                )

    layers = sec_ref[...]
    first = jnp.sum((layers < s).astype(jnp.int32), axis=1, keepdims=True) * kinds
    last = jnp.sum((layers <= s).astype(jnp.int32), axis=1, keepdims=True) * kinds
    column = lax.broadcasted_iota(jnp.int32, (1, LT), 1)
    owned = (column >= first) & (column < last)

    for p in other_pairs:
        arrived(mxbuf.at[p], mx_send.at[p], mx_recv.at[p])
    merged = obs_ref[...]
    for p in other_pairs:
        merged = jnp.maximum(merged, mxbuf[p])
    m1buf[...] = jnp.where(owned, merged, 0.0)
    for k, (sec, dp) in enumerate(others_sc):
        send(
            m1buf, mcbuf.at[2 * s + core], mc_send.at[k], mc_recv.at[2 * s + core],
            dev(dp=dp, section=sec),
        )

    def from_other_pairs(k):
        for p in other_pairs:
            if k == 0:
                e = 2 * p + core
                arrived(shard(e, t), gx_send.at[p], gx_recv.at[p])
                pass_on(None, p, t, True, always)
                pass_on(None, p, t, False, always)
                send(shard(e, t), shard(e, t), gc_send.at[p, t], gc_recv.at[p, t], dev(dp=partner))
            else:
                relay(p, k)

    for sec, dp in others_sc:
        slot = 2 * sec + lax.rem(dp, 2)
        arrived(mcbuf.at[slot], mc_send.at[0], mc_recv.at[slot])
    merged = m1buf[...]
    for sec, dp in others_sc:
        merged = jnp.maximum(merged, mcbuf[2 * sec + lax.rem(dp, 2)])
    m2buf[...] = merged
    for tt in other_t:
        send(m2buf, mzbuf.at[t], mz_send.at[tt], mz_recv.at[t], dev(tensor=tt))

    load_hist.wait()
    roll = roll_ref[0]
    slot_id = lax.broadcasted_iota(jnp.int32, (slots, 1), 0)
    lane_id = lax.broadcasted_iota(jnp.int32, (1, slots), 1)
    age = roll - slot_id
    age = jnp.where(age < 0, age + slots, age)
    best_x = jnp.zeros((1, 1), jnp.float32)
    best_g = jnp.zeros((1, 1), jnp.float32)
    in_x = (age >= 1) & (age <= len_ref[0])
    in_g = (age >= 1) & (age <= len_ref[1])
    blocks = [(b, b + LANES) for b in range(0, LT, LANES)]
    for lo, hi in blocks:
        h = hbuf[lo:hi, :].T
        col = lo + lax.broadcasted_iota(jnp.int32, (1, hi - lo), 1)
        group = jnp.floor((col.astype(jnp.float32) + 0.5) * (1.0 / kinds)).astype(jnp.int32)
        kind = col - group * kinds
        length = jnp.zeros((1, hi - lo), jnp.int32)
        for i in range(kinds):
            length = jnp.where(kind == i, len_ref[i], length)
        window = (age >= 1) & (age < length)
        pre[:, lo:hi] = jnp.max(jnp.where(window, h, 0.0), axis=0, keepdims=True)
        hx = jnp.max(jnp.where(in_x, h, 0.0), axis=0, keepdims=True)
        hg = jnp.max(jnp.where(in_g, h, 0.0), axis=0, keepdims=True)
        best_x = jnp.maximum(
            best_x, jnp.max(jnp.where(col == first, hx, 0.0), axis=1, keepdims=True)
        )
        best_g = jnp.maximum(
            best_g, jnp.max(jnp.where(col == first + 1, hg, 0.0), axis=1, keepdims=True)
        )
    sx = FP8_MAX / best_x
    sg = FP8_MAX / best_g
    inverse = 1.0 / (sx * sg)

    load_grads.wait()
    for k in range(1, nt):
        relay(pair, k)
        if k < nt:
            from_other_pairs(k - 1)

    for tt in other_t:
        arrived(mzbuf.at[tt], mz_send.at[tt], mz_recv.at[tt])
    merged = m2buf[...]
    for tt in other_t:
        merged = jnp.maximum(merged, mzbuf[tt])
    mine[:, 0:LT] = merged
    ns_ref[...] = FP8_MAX / jnp.maximum(pre[:, 0:LT], merged)
    for lo, hi in blocks:
        row = jnp.broadcast_to(mine[:, lo:hi], (slots, hi - lo)).T
        hout[lo:hi, :] = jnp.where(lane_id == roll, row, hbuf[lo:hi, :])
    store_hist = pltpu.make_async_copy(hout.at[pl.ds(0, LT), :], nh_ref, local_sem.at[3])
    store_hist.start()

    def rows_of(p):
        return pl.ds(pl.multiple_of(p * 2 * T, 2 * T), 2 * T)

    def grads_of(p):
        for tt in range(nt):
            arrived(shard(2 * p + 1 - core, tt), gc_send.at[p, tt], gc_recv.at[p, tt])
        for tt in range(nt):
            gq[rows_of(p), tt * gw:(tt + 1) * gw] = quantize(gbuf[tt, rows_of(p), :], sg)

    def product(p, lo, n):
        a = quantize(abuf[rows_of(p), lo:lo + n], sx)
        return lax.dot_general(
            a, gq[rows_of(p), :], (((0,), (0,)), ((), ())), preferred_element_type=jnp.float32
        )

    load_acts.wait()
    arrived(abuf.at[pl.ds(pl.multiple_of(partner * T, T), T), :], ap_sem.at[0], ap_sem.at[1])
    grads_of(pair)
    for lo in range(0, w, cw):
        acc[lo:lo + cw, :] = product(pair, lo, cw)
    from_other_pairs(nt - 1)
    for p in other_pairs:
        grads_of(p)
    stores = []
    for q, (lo, n) in enumerate(spans):
        span = slice(lo, lo + n)
        for j, p in enumerate(other_pairs):
            for c in range(2):
                src = 2 * p + c
                arrived(
                    abuf.at[pl.ds(pl.multiple_of(src * T, T), T), pl.ds(lo, n)],
                    a_send.at[q, src], a_recv.at[q, src],
                )
            acc[span, :] += product(p, lo, n)
        obuf[span, :] = (acc[span, :] * inverse).astype(jnp.bfloat16)
        store = pltpu.make_async_copy(obuf.at[span, :], w_ref.at[span, :], local_sem.at[4 + q])
        store.start()
        stores.append(store)
    store_hist.wait()
    for copy in sends:
        copy.wait_send()
    for cond, src, p, origin, right in passed:
        pl.when(cond)(lambda: along(src, p, origin, right).wait_send())
    for p in [pair] + other_pairs:
        for k in range(1, nt):
            for origin, has in ((t - k, t - k >= 0), (t + k, t + k < nt)):
                pl.when(has)(lambda: to_core(p, origin).wait_send())
    for store in stores:
        store.wait()


def hand_over(scale_ref, hist_ref, w_ref, ns_ref, nh_ref, wout_ref, hbuf, wbuf, in_sem, out_sem):
    rows, cut = w_ref.shape[0], hist_ref.shape[0] // 16 * 8
    step = max(rows // 4, 16)
    spans = [(w_ref, wbuf, wout_ref, lo, step) for lo in range(0, rows, step)]
    spans.append((hist_ref, hbuf, nh_ref, 0, cut))
    spans.append((hist_ref, hbuf, nh_ref, cut, hist_ref.shape[0] - cut))
    reads, writes = [], []
    for i, (src, held, dst, lo, n) in enumerate(spans):
        span = pl.ds(lo, n)
        reads.append(pltpu.make_async_copy(src.at[span, :], held.at[span, :], in_sem.at[i]))
        writes.append(pltpu.make_async_copy(held.at[span, :], dst.at[span, :], out_sem.at[i]))
    for read in reads:
        read.start()
    ns_ref[...] = scale_ref[...].reshape(ns_ref.shape)
    for read, write in zip(reads, writes):
        read.wait()
        write.start()
    for write in writes:
        write.wait()


def solution(mesh):
    ndp, nsec, nt = mesh.shape["dp"], mesh.shape["section"], mesh.shape["tensor"]

    def body(observed, section_of, hist_len, roll_index, history, acts, grads):
        slots, LT = history.shape
        T, cols = acts.shape[1:]
        gw = grads.shape[2]
        w = cols // ndp
        cw = min(w, 256)
        nq = len(chunks(w, cw))
        npair = ndp // 2
        kv = gw * nt
        padded = pl.cdiv(LT, LANES) * LANES
        f32, bf16 = jnp.float32, jnp.bfloat16
        dma = pltpu.SemaphoreType.DMA
        hbm = pl.BlockSpec(memory_space=pltpu.HBM)
        any_spec = pl.BlockSpec(memory_space=pl.ANY)
        vmem = pl.BlockSpec(memory_space=pltpu.VMEM)
        smem = pl.BlockSpec(memory_space=pltpu.SMEM)
        new_history, new_scale, wgrad = pl.pallas_call(
            functools.partial(kernel, ndp, nsec, nt, cw),
            out_shape=(
                jax.ShapeDtypeStruct((LT, slots), f32),
                jax.ShapeDtypeStruct((1, LT), f32),
                jax.ShapeDtypeStruct((w, kv), bf16),
            ),
            in_specs=[smem, smem, vmem, vmem, hbm, hbm, hbm],
            out_specs=(any_spec, vmem, any_spec),
            scratch_shapes=[
                pltpu.VMEM((ndp * T, w), bf16),
                pltpu.VMEM((nt, ndp * T, gw), bf16),
                pltpu.VMEM((ndp * T, kv), bf16),
                pltpu.VMEM((w, kv), f32),
                pltpu.VMEM((w, kv), bf16),
                pltpu.VMEM((padded, slots), f32),
                pltpu.VMEM((padded, slots), f32),
                pltpu.VMEM((1, padded), f32),
                pltpu.VMEM((1, padded), f32),
                pltpu.VMEM((npair, 1, LT), f32),
                pltpu.VMEM((1, LT), f32),
                pltpu.VMEM((2 * nsec, 1, LT), f32),
                pltpu.VMEM((1, LT), f32),
                pltpu.VMEM((nt, 1, LT), f32),
                dma((4 + nq,)),
                dma((2,)),
                dma((nq, ndp)),
                dma((nq, ndp)),
                dma((npair,)),
                dma((npair,)),
                dma((npair, nt)),
                dma((npair, nt)),
                dma((npair, nt)),
                dma((npair, nt)),
                dma((npair, nt)),
                dma((npair,)),
                dma((npair,)),
                dma((2 * nsec,)),
                dma((2 * nsec,)),
                dma((nt,)),
                dma((nt,)),
            ],
            compiler_params=pltpu.CompilerParams(
                collective_id=0, has_side_effects=True, vmem_limit_bytes=60 * 1024 * 1024
            ),
            name="merge_and_grad",
        )(
            roll_index.reshape(1), hist_len, section_of.reshape(1, -1),
            observed.reshape(1, LT), history.T, acts[0], grads[0],
        )
        new_scale, new_history, wgrad = pl.pallas_call(
            hand_over,
            out_shape=(
                jax.ShapeDtypeStruct((LT,), f32),
                jax.ShapeDtypeStruct((LT, slots), f32),
                jax.ShapeDtypeStruct((w, kv), bf16),
            ),
            in_specs=[vmem, any_spec, any_spec],
            out_specs=(vmem, any_spec, any_spec),
            scratch_shapes=[
                pltpu.VMEM((LT, slots), f32),
                pltpu.VMEM((w, kv), bf16),
                dma((8,)),
                dma((8,)),
            ],
            compiler_params=pltpu.CompilerParams(vmem_limit_bytes=60 * 1024 * 1024),
            name="hand_over",
        )(new_scale, new_history, wgrad)
        return new_history.T, new_scale, wgrad[None]

    in_specs = (
        P("dp", "section", "tensor", None),
        P(),
        P(),
        P(),
        P(),
        P("section", "dp", "tensor"),
        P("section", "dp", "tensor"),
    )
    out_specs = (P(), P(), P("section", ("tensor", "dp"), None))
    return jax.shard_map(body, mesh=mesh, in_specs=in_specs, out_specs=out_specs, check_vma=False)
```
